512 devices in a mesh: groups: 2 (over y), mp: 16 (over z), dp: 8 (over x), guide: 2 (over core).
Axes of the slice: x: 8, y: 2, z: 16, core: 2. Of those that a mesh axis runs over, the one named last changes fastest.
The devices are a block of a 8x8x16 slice.
Arguments:
- tokens: bfloat16 [768, 8192], P(('groups', 'mp'), ('dp', 'guide')), parts along dimension 0, may hold values from -6 to 6
- w_gate: bfloat16 [8192, 14336], P(('dp', 'guide'), 'mp'), may hold values from -0.0625 to 0.0625
- w_up: bfloat16 [8192, 14336], P(('dp', 'guide'), 'mp'), may hold values from -0.0625 to 0.0625
- w_down: bfloat16 [14336, 8192], P('mp', ('dp', 'guide')), may hold values from -0.046875 to 0.046875
Outputs:
- layer_output: bfloat16 [768, 8192], P(('groups', 'mp'), ('dp', 'guide')), parts along dimension 0
The draws below stay inside these ranges and needn't reach their ends.
There are 2 independent parts, one for each index of `groups`. The reference program is written for one: setup_inputs(seed, part) draws one part's arguments, and reference() takes and returns one part's arrays. A program takes and returns all parts, laid end to end along the dimension named above; an argument that names none is the same for every part. Nothing has to cross between parts.
All inputs are finite; a program needn't handle non-finite values.
Results may differ from the reference program's by a relative error of at most 0.0049.
Values may be sent and summed in bfloat16 or wider, within the bound.
No kernel may reach another device: no remote copies, remote signals or barrier semaphores. Data moves between devices by JAX's collectives and lax.ppermute only.
A program may use at most 64 MiB of HBM per device.

```python
import jax
import jax.numpy as jnp

D = 8192
FF = 14336
ROWS = 384


def level_of(own_key, shape, split, least, largest):
    level, own = 1.0, jax.random.fold_in(own_key, 6)
    for dim, parts in split:
        steps = jnp.exp(jax.random.uniform(jax.random.fold_in(own, dim), (parts,), jnp.float32, least / len(split), largest / len(split)))
        level = level * jnp.repeat(steps, shape[dim] // parts).reshape([-1 if axis == dim else 1 for axis in range(len(shape))])
    return level


def gaussian(key, dims, deviation, reach, cuts=(), dtype=jnp.bfloat16):
    result = jax.random.normal(key, dims, jnp.float32) * deviation
    if len(cuts) > 0:
        result = level_of(key, dims, cuts, -0.22, 0.18) * result
    return jnp.clip(result, min=-reach, max=reach).astype(dtype)


def setup_inputs(seed: int = 0, part: int = 0) -> dict:
    splits = jax.random.split(jax.random.key(seed), 5)
    part_keys = jax.random.split(jax.random.fold_in(splits[4], part), 5)
    tokens = gaussian(part_keys[0], (ROWS, D), 1.0, 6.0, ((0, 16), (1, 16)))
    w_gate = gaussian(splits[1], (D, FF), D ** -0.5, 0.0625, ((0, 16), (1, 16)))
    w_up = gaussian(splits[2], (D, FF), D ** -0.5, 0.0625, ((0, 16), (1, 16)))
    w_down = gaussian(splits[3], (FF, D), FF ** -0.5, 0.046875, ((0, 16), (1, 16)))
    return dict(tokens=tokens, w_gate=w_gate, w_up=w_up, w_down=w_down)


def reference(tokens, w_gate, w_up, w_down):
    gate_sum = jnp.dot(tokens, w_gate, preferred_element_type=jnp.float32)
    up_sum = jnp.dot(tokens, w_up, preferred_element_type=jnp.float32)
    hidden = (jax.nn.silu(gate_sum) * up_sum).astype(jnp.bfloat16)
    total = jnp.dot(hidden, w_down, preferred_element_type=jnp.float32)
    return total.astype(jnp.bfloat16)
```

```python
import jax
import jax.numpy as jnp
from jax import lax
from jax.sharding import PartitionSpec as P


def summed_on_arrival(tiles, axis):
    arrived = lax.all_to_all(tiles, axis, split_axis=0, concat_axis=0, tiled=True)
    return arrived.astype(jnp.float32).sum(axis=0)


def cut(shard, count):
    return shard.reshape(count, shard.shape[0] // count, *shard.shape[1:])


def per_device(tokens, w_gate, w_up, w_down):
    columns = w_gate.shape[1]
    mp, dp, guide = (lax.axis_size(axis) for axis in ("mp", "dp", "guide"))
    paired_weights = jnp.concatenate([w_gate, w_up], axis=1)
    blocks = lax.all_gather(tokens, "mp", axis=0, tiled=False)
    blocks = blocks.reshape(dp, guide, -1, *tokens.shape)
    gathered = blocks.swapaxes(0, 1).reshape(-1, tokens.shape[1])
    partial_terms = jnp.dot(gathered, paired_weights, preferred_element_type=jnp.float32)
    chip_terms = summed_on_arrival(cut(partial_terms, guide), "guide").astype(jnp.bfloat16)
    summed = summed_on_arrival(cut(chip_terms, dp), "dp")
    hidden_share = (jax.nn.silu(summed[:, :columns]) * summed[:, columns:]).astype(jnp.bfloat16)
    hidden = lax.all_gather(hidden_share, ("dp", "guide"), axis=0, tiled=True)
    output_terms = jnp.dot(hidden, w_down, preferred_element_type=jnp.float32).astype(jnp.bfloat16)
    return summed_on_arrival(cut(output_terms, mp), "mp").astype(jnp.bfloat16)


def solution(mesh):
    placed = (
        P(("groups", "mp"), ("dp", "guide")),
        P(("dp", "guide"), "mp"),
        P(("dp", "guide"), "mp"),
        P("mp", ("dp", "guide")),
    )
    return jax.shard_map(
        per_device,
        mesh=mesh,
        in_specs=placed,
        out_specs=P(("groups", "mp"), ("dp", "guide")),
        check_vma=False,
    )
```

```python
import jax
import jax.numpy as jnp
from jax import lax
from jax.sharding import PartitionSpec as P


def summed_on_arrival(tiles, axis):
    arrived = lax.all_to_all(tiles, axis, split_axis=0, concat_axis=0, tiled=True)
    total = arrived[0].astype(jnp.float32)
    for tile in arrived[1:]:
        total = total + tile.astype(jnp.float32)
    return total


def from_other_core(array):
    count = lax.axis_size("guide")
    return lax.ppermute(array, "guide", [(core, (core + 1) % count) for core in range(count)])


def per_device(tokens, w_gate, w_up, w_down):
    columns = w_gate.shape[1]
    rows, features = tokens.shape
    mp, dp, guide = (lax.axis_size(axis) for axis in ("mp", "dp", "guide"))
    core = lax.axis_index("guide")
    own_weights = jnp.concatenate([w_gate, w_up], axis=1)
    other_weights = jnp.concatenate([from_other_core(w_gate), from_other_core(w_up)], axis=1)
    blocks = lax.all_gather(tokens, ("mp", "guide"), axis=0, tiled=False)
    blocks = blocks.reshape(dp, guide, guide, rows, features)
    mine = lax.dynamic_index_in_dim(blocks, core, 1, keepdims=False)
    own = lax.dynamic_index_in_dim(mine, core, 1, keepdims=False).reshape(-1, features)
    other = lax.dynamic_index_in_dim(mine, 1 - core, 1, keepdims=False).reshape(-1, features)
    chip_terms = jnp.dot(own, own_weights, preferred_element_type=jnp.float32) + jnp.dot(
        other, other_weights, preferred_element_type=jnp.float32
    )
    chip_terms = chip_terms.astype(jnp.bfloat16).reshape(dp, rows, -1)
    summed = summed_on_arrival(chip_terms, "dp")
    hidden_share = (jax.nn.silu(summed[:, :columns]) * summed[:, columns:]).astype(jnp.bfloat16)
    hidden = lax.all_gather(hidden_share, ("dp", "guide"), axis=0, tiled=True)
    output_terms = jnp.dot(hidden, w_down, preferred_element_type=jnp.float32).astype(jnp.bfloat16)
    return summed_on_arrival(output_terms.reshape(mp, rows, -1), "mp").astype(jnp.bfloat16)


def solution(mesh):
    placed = (
        P(("groups", "mp"), ("dp", "guide")),
        P(("dp", "guide"), "mp"),
        P(("dp", "guide"), "mp"),
        P("mp", ("dp", "guide")),
    )
    return jax.shard_map(
        per_device,
        mesh=mesh,
        in_specs=placed,
        out_specs=P(("groups", "mp"), ("dp", "guide")),
        check_vma=False,
    )
```

```python
import jax
import jax.numpy as jnp
from jax import lax
from jax.sharding import PartitionSpec as P


def summed_on_arrival(tiles, axis):
    arrived = lax.all_to_all(tiles, axis, split_axis=0, concat_axis=0, tiled=True)
    total = arrived[0].astype(jnp.float32)
    for tile in arrived[1:]:
        total = total + tile.astype(jnp.float32)
    return total


def from_other_core(array):
    count = lax.axis_size("guide")
    return lax.ppermute(array, "guide", [(core, (core + 1) % count) for core in range(count)])


def per_device(tokens, w_gate, w_up, w_down):
    columns = w_gate.shape[1]
    rows, features = tokens.shape
    mp, dp, guide = (lax.axis_size(axis) for axis in ("mp", "dp", "guide"))
    core = lax.axis_index("guide")
    own_weights = lax.optimization_barrier(jnp.concatenate([w_gate, w_up], axis=1))
    other_weights = from_other_core(own_weights)
    blocks = lax.all_gather(tokens, ("mp", "guide"), axis=0, tiled=False)
    blocks = blocks.reshape(dp, guide, guide, rows, features)
    mine = lax.dynamic_index_in_dim(blocks, core, 1, keepdims=False)
    own = lax.dynamic_index_in_dim(mine, core, 1, keepdims=False).reshape(-1, features)
    other = lax.dynamic_index_in_dim(mine, 1 - core, 1, keepdims=False).reshape(-1, features)
    chip_terms = jnp.dot(own, own_weights, preferred_element_type=jnp.float32) + jnp.dot(
        other, other_weights, preferred_element_type=jnp.float32
    )
    chip_terms = chip_terms.astype(jnp.bfloat16).reshape(dp, rows, -1)
    summed = summed_on_arrival(chip_terms, "dp")
    hidden_share = (jax.nn.silu(summed[:, :columns]) * summed[:, columns:]).astype(jnp.bfloat16)
    hidden = lax.all_gather(hidden_share, ("dp", "guide"), axis=0, tiled=True)
    output_terms = jnp.dot(hidden, w_down, preferred_element_type=jnp.float32).astype(jnp.bfloat16)
    return summed_on_arrival(output_terms.reshape(mp, rows, -1), "mp").astype(jnp.bfloat16)


def solution(mesh):
    placed = (
        P(("groups", "mp"), ("dp", "guide")),
        P(("dp", "guide"), "mp"),
        P(("dp", "guide"), "mp"),
        P("mp", ("dp", "guide")),
    )
    return jax.shard_map(
        per_device,
        mesh=mesh,
        in_specs=placed,
        out_specs=P(("groups", "mp"), ("dp", "guide")),
        check_vma=False,
    )
```

```python
import jax
import jax.numpy as jnp
from jax import lax
from jax.sharding import PartitionSpec as P


def summed_on_arrival(tiles, axis):
    arrived = lax.all_to_all(tiles, axis, split_axis=0, concat_axis=0, tiled=True)
    total = arrived[0].astype(jnp.float32)
    for tile in arrived[1:]:
        total = total + tile.astype(jnp.float32)
    return total


def from_other_core(array):
    count = lax.axis_size("guide")
    return lax.ppermute(array, "guide", [(core, (core + 1) % count) for core in range(count)])


def per_device(tokens, w_gate, w_up, w_down):
    columns = w_gate.shape[1]
    rows, features = tokens.shape
    mp, dp, guide = (lax.axis_size(axis) for axis in ("mp", "dp", "guide"))
    core = lax.axis_index("guide")
    paired_weights = jnp.concatenate([w_gate, w_up], axis=1)
    blocks = lax.all_gather(tokens, "mp", axis=0, tiled=False)
    blocks = blocks.reshape(dp, guide, rows, features)

    def terms(owner):
        owned = lax.dynamic_index_in_dim(blocks, owner, 1, keepdims=False)
        return jnp.dot(
            owned.reshape(-1, features), paired_weights, preferred_element_type=jnp.float32
        )

    received = from_other_core(terms(1 - core))
    own = lax.optimization_barrier(terms(core))
    chip_terms = (own + received).astype(jnp.bfloat16).reshape(dp, rows, -1)
    summed = summed_on_arrival(chip_terms, "dp")
    hidden_share = (jax.nn.silu(summed[:, :columns]) * summed[:, columns:]).astype(jnp.bfloat16)
    hidden = lax.all_gather(hidden_share, ("dp", "guide"), axis=0, tiled=True)
    output_terms = jnp.dot(hidden, w_down, preferred_element_type=jnp.float32).astype(jnp.bfloat16)
    return summed_on_arrival(output_terms.reshape(mp, rows, -1), "mp").astype(jnp.bfloat16)


def solution(mesh):
    placed = (
        P(("groups", "mp"), ("dp", "guide")),
        P(("dp", "guide"), "mp"),
        P(("dp", "guide"), "mp"),
        P("mp", ("dp", "guide")),
    )
    return jax.shard_map(
        per_device,
        mesh=mesh,
        in_specs=placed,
        out_specs=P(("groups", "mp"), ("dp", "guide")),
        check_vma=False,
    )
```

```python
import jax
import jax.numpy as jnp
from jax import lax
from jax.sharding import PartitionSpec as P


def summed_on_arrival(tiles, axis):
    arrived = lax.all_to_all(tiles, axis, split_axis=0, concat_axis=0, tiled=True)
    total = arrived[0].astype(jnp.float32)
    for tile in arrived[1:]:
        total = total + tile.astype(jnp.float32)
    return total


def from_other_core(array):
    count = lax.axis_size("guide")
    return lax.ppermute(array, "guide", [(core, (core + 1) % count) for core in range(count)])


def per_device(tokens, w_gate, w_up, w_down):
    columns = w_gate.shape[1]
    rows, features = tokens.shape
    mp, dp, guide = (lax.axis_size(axis) for axis in ("mp", "dp", "guide"))
    core = lax.axis_index("guide")
    blocks = lax.all_gather(tokens, "mp", axis=0, tiled=False)
    blocks = blocks.reshape(dp, guide, rows, features)

    def terms(owner):
        owned = lax.dynamic_index_in_dim(blocks, owner, 1, keepdims=False).reshape(-1, features)
        return jnp.concatenate(
            [jnp.dot(owned, w, preferred_element_type=jnp.float32) for w in (w_gate, w_up)], axis=1
        )

    received = from_other_core(terms(1 - core))
    own = lax.optimization_barrier(terms(core))
    chip_terms = (own + received).astype(jnp.bfloat16).reshape(dp, rows, -1)
    summed = summed_on_arrival(chip_terms, "dp")
    hidden_share = (jax.nn.silu(summed[:, :columns]) * summed[:, columns:]).astype(jnp.bfloat16)
    hidden = lax.all_gather(hidden_share, ("dp", "guide"), axis=0, tiled=True)
    output_terms = jnp.dot(hidden, w_down, preferred_element_type=jnp.float32).astype(jnp.bfloat16)
    return summed_on_arrival(output_terms.reshape(mp, rows, -1), "mp").astype(jnp.bfloat16)


def solution(mesh):
    placed = (
        P(("groups", "mp"), ("dp", "guide")),
        P(("dp", "guide"), "mp"),
        P(("dp", "guide"), "mp"),
        P("mp", ("dp", "guide")),
    )
    return jax.shard_map(
        per_device,
        mesh=mesh,
        in_specs=placed,
        out_specs=P(("groups", "mp"), ("dp", "guide")),
        check_vma=False,
    )
```

```python
import jax
import jax.numpy as jnp
from jax import lax
from jax.sharding import PartitionSpec as P


def summed_on_arrival(tiles, axis):
    arrived = lax.all_to_all(tiles, axis, split_axis=0, concat_axis=0, tiled=True)
    total = arrived[0].astype(jnp.float32)
    for tile in arrived[1:]:
        total = total + tile.astype(jnp.float32)
    return total


def from_other_core(array):
    count = lax.axis_size("guide")
    return lax.ppermute(array, "guide", [(core, (core + 1) % count) for core in range(count)])


def per_device(tokens, w_gate, w_up, w_down):
    columns = w_gate.shape[1]
    rows, features = tokens.shape
    mp, dp, guide = (lax.axis_size(axis) for axis in ("mp", "dp", "guide"))
    core = lax.axis_index("guide")
    head = 2 * rows // 3
    tail = rows - head
    own_parity = lax.axis_index("mp") % guide == core
    other_tokens = from_other_core(tokens)
    both = jnp.stack([tokens, other_tokens])
    own_weights = lax.optimization_barrier(jnp.concatenate([w_gate, w_up], axis=1))
    other_weights = from_other_core(own_weights)
    owned = jnp.where(
        own_parity,
        both[:, :head],
        jnp.pad(both[:, head:], ((0, 0), (0, head - tail), (0, 0))),
    )
    blocks = lax.all_gather(owned.reshape(-1, features), "mp", axis=0, tiled=True)
    blocks = blocks.reshape(dp, guide, 2, head, features)
    heads = lax.dynamic_index_in_dim(blocks, core, 1, keepdims=False)
    tails = lax.dynamic_index_in_dim(blocks, 1 - core, 1, keepdims=False)[:, :, :tail]
    mine = jnp.concatenate([heads, tails], axis=2)
    chip_terms = jnp.dot(
        mine[:, 0].reshape(-1, features), own_weights, preferred_element_type=jnp.float32
    ) + jnp.dot(
        mine[:, 1].reshape(-1, features), other_weights, preferred_element_type=jnp.float32
    )
    summed = summed_on_arrival(chip_terms.astype(jnp.bfloat16).reshape(dp, rows, -1), "dp")
    hidden_share = (jax.nn.silu(summed[:, :columns]) * summed[:, columns:]).astype(jnp.bfloat16)
    hidden = lax.all_gather(hidden_share, ("dp", "guide"), axis=0, tiled=True)
    output_terms = jnp.dot(hidden, w_down, preferred_element_type=jnp.float32).astype(jnp.bfloat16)
    output_terms = output_terms.reshape(dp, guide, rows, -1)
    placed = jnp.concatenate(
        [output_terms[:, :, :head], output_terms[:, ::-1, head:]], axis=2
    )
    return summed_on_arrival(placed.reshape(mp, rows, -1), "mp").astype(jnp.bfloat16)


def solution(mesh):
    placed = (
        P(("groups", "mp"), ("dp", "guide")),
        P(("dp", "guide"), "mp"),
        P(("dp", "guide"), "mp"),
        P("mp", ("dp", "guide")),
    )
    return jax.shard_map(
        per_device,
        mesh=mesh,
        in_specs=placed,
        out_specs=P(("groups", "mp"), ("dp", "guide")),
        check_vma=False,
    )
```

```python
import jax
import jax.numpy as jnp
from jax import lax
from jax.sharding import PartitionSpec as P


def summed_on_arrival(tiles, axis):
    arrived = lax.all_to_all(tiles, axis, split_axis=0, concat_axis=0, tiled=True)
    total = arrived[0].astype(jnp.float32)
    for tile in arrived[1:]:
        total = total + tile.astype(jnp.float32)
    return total


def from_other_core(array):
    count = lax.axis_size("guide")
    return lax.ppermute(array, "guide", [(core, (core + 1) % count) for core in range(count)])


def per_device(tokens, w_gate, w_up, w_down):
    columns = w_gate.shape[1]
    rows, features = tokens.shape
    mp, dp, guide = (lax.axis_size(axis) for axis in ("mp", "dp", "guide"))
    core = lax.axis_index("guide")
    head = 2 * rows // 3
    tail = rows - head
    own_parity = lax.axis_index("mp") % guide == core
    other_tokens = from_other_core(tokens)
    both = jnp.stack([tokens, other_tokens])
    own_weights = lax.optimization_barrier(jnp.concatenate([w_gate, w_up], axis=1))
    other_weights = from_other_core(own_weights)
    other_w_down = from_other_core(w_down)
    owned = jnp.where(
        own_parity,
        both[:, :head],
        jnp.pad(both[:, head:], ((0, 0), (0, head - tail), (0, 0))),
    )
    blocks = lax.all_gather(owned.reshape(-1, features), "mp", axis=0, tiled=True)
    blocks = blocks.reshape(dp, guide, 2, head, features)
    heads = lax.dynamic_index_in_dim(blocks, core, 1, keepdims=False)
    tails = lax.dynamic_index_in_dim(blocks, 1 - core, 1, keepdims=False)[:, :, :tail]
    mine = jnp.concatenate([heads, tails], axis=2)
    chip_terms = jnp.dot(
        mine[:, 0].reshape(-1, features), own_weights, preferred_element_type=jnp.float32
    ) + jnp.dot(
        mine[:, 1].reshape(-1, features), other_weights, preferred_element_type=jnp.float32
    )
    summed = summed_on_arrival(chip_terms.astype(jnp.bfloat16).reshape(dp, rows, -1), "dp")
    hidden_share = (jax.nn.silu(summed[:, :columns]) * summed[:, columns:]).astype(jnp.bfloat16)
    copies = jnp.broadcast_to(hidden_share[None], (dp, *hidden_share.shape))
    hidden = lax.all_to_all(copies, "dp", 0, 0, tiled=True).reshape(dp * rows, columns)
    hidden, core = lax.optimization_barrier((hidden, core))
    halves = jnp.stack(
        [
            jnp.dot(hidden, w, preferred_element_type=jnp.float32)
            .astype(jnp.bfloat16)
            .reshape(dp, rows, -1)
            for w in (w_down, other_w_down)
        ],
        axis=1,
    )
    tiles = jnp.where(
        (jnp.arange(guide) == core)[None, :, None, None, None],
        halves[:, None, :, :head],
        jnp.pad(halves[:, None, :, head:], ((0, 0), (0, 0), (0, 0), (0, head - tail), (0, 0))),
    )
    output_rows = summed_on_arrival(tiles.reshape(mp, 2 * head, -1), "mp").astype(jnp.bfloat16)
    kept, received = output_rows[:head], from_other_core(output_rows[head:])
    return jnp.where(
        own_parity,
        jnp.concatenate([kept, received[:tail]], axis=0),
        jnp.concatenate([received, kept[:tail]], axis=0),
    )


def solution(mesh):
    placed = (
        P(("groups", "mp"), ("dp", "guide")),
        P(("dp", "guide"), "mp"),
        P(("dp", "guide"), "mp"),
        P("mp", ("dp", "guide")),
    )
    return jax.shard_map(
        per_device,
        mesh=mesh,
        in_specs=placed,
        out_specs=P(("groups", "mp"), ("dp", "guide")),
        check_vma=False,
    )
```

```python
import jax
import jax.numpy as jnp
from jax import lax
from jax.sharding import PartitionSpec as P


def summed_on_arrival(tiles, axis):
    arrived = lax.all_to_all(tiles, axis, split_axis=0, concat_axis=0, tiled=True)
    total = arrived[0].astype(jnp.float32)
    for tile in arrived[1:]:
        total = total + tile.astype(jnp.float32)
    return total


def from_other_core(array):
    count = lax.axis_size("guide")
    return lax.ppermute(array, "guide", [(core, (core + 1) % count) for core in range(count)])


def per_device(tokens, w_gate, w_up, w_down):
    columns = w_gate.shape[1]
    rows, features = tokens.shape
    mp, dp, guide = (lax.axis_size(axis) for axis in ("mp", "dp", "guide"))
    core = lax.axis_index("guide")
    head = 2 * rows // 3
    tail = rows - head
    own_parity = lax.axis_index("mp") % guide == core
    other_tokens = from_other_core(tokens)
    both = jnp.stack([tokens, other_tokens])
    other_gate = from_other_core(w_gate)
    other_up = from_other_core(w_up)
    other_w_down = from_other_core(w_down)
    owned = jnp.where(
        own_parity,
        both[:, :head],
        jnp.pad(both[:, head:], ((0, 0), (0, head - tail), (0, 0))),
    )
    blocks = lax.all_gather(owned.reshape(-1, features), "mp", axis=0, tiled=True)
    blocks = blocks.reshape(dp, guide, 2, head, features)
    heads = lax.dynamic_index_in_dim(blocks, core, 1, keepdims=False)
    tails = lax.dynamic_index_in_dim(blocks, 1 - core, 1, keepdims=False)[:, :, :tail]
    mine = jnp.concatenate([heads, tails], axis=2)
    own_rows, other_rows = (mine[:, half].reshape(-1, features) for half in range(2))
    other_terms = [
        jnp.dot(other_rows, w, preferred_element_type=jnp.float32) for w in (other_gate, other_up)
    ]
    own_rows, other_terms = lax.optimization_barrier((own_rows, other_terms))
    chip_terms = jnp.concatenate(
        [
            (terms + jnp.dot(own_rows, w, preferred_element_type=jnp.float32)).astype(jnp.bfloat16)
            for terms, w in zip(other_terms, (w_gate, w_up))
        ],
        axis=1,
    )
    summed = summed_on_arrival(chip_terms.reshape(dp, rows, -1), "dp")
    hidden_share = (jax.nn.silu(summed[:, :columns]) * summed[:, columns:]).astype(jnp.bfloat16)
    copies = jnp.broadcast_to(hidden_share[None], (dp, *hidden_share.shape))
    hidden = lax.all_to_all(copies, "dp", 0, 0, tiled=True).reshape(dp * rows, columns)
    hidden, core = lax.optimization_barrier((hidden, core))
    halves = jnp.stack(
        [
            jnp.dot(hidden, w, preferred_element_type=jnp.float32)
            .astype(jnp.bfloat16)
            .reshape(dp, rows, -1)
            for w in (w_down, other_w_down)
        ],
        axis=1,
    )
    tiles = jnp.where(
        (jnp.arange(guide) == core)[None, :, None, None, None],
        halves[:, None, :, :head],
        jnp.pad(halves[:, None, :, head:], ((0, 0), (0, 0), (0, 0), (0, head - tail), (0, 0))),
    )
    output_rows = summed_on_arrival(tiles.reshape(mp, 2 * head, -1), "mp").astype(jnp.bfloat16)
    kept, received = output_rows[:head], from_other_core(output_rows[head:])
    return jnp.where(
        own_parity,
        jnp.concatenate([kept, received[:tail]], axis=0),
        jnp.concatenate([received, kept[:tail]], axis=0),
    )


def solution(mesh):
    placed = (
        P(("groups", "mp"), ("dp", "guide")),
        P(("dp", "guide"), "mp"),
        P(("dp", "guide"), "mp"),
        P("mp", ("dp", "guide")),
    )
    return jax.shard_map(
        per_device,
        mesh=mesh,
        in_specs=placed,
        out_specs=P(("groups", "mp"), ("dp", "guide")),
        check_vma=False,
    )
```

```python
import jax
import jax.numpy as jnp
from jax import lax
from jax.sharding import PartitionSpec as P


def summed_on_arrival(tiles, axis):
    arrived = lax.all_to_all(tiles, axis, split_axis=0, concat_axis=0, tiled=True)
    total = arrived[0].astype(jnp.float32)
    for tile in arrived[1:]:
        total = total + tile.astype(jnp.float32)
    return total


def from_other_core(array):
    count = lax.axis_size("guide")
    return lax.ppermute(array, "guide", [(core, (core + 1) % count) for core in range(count)])


def per_device(tokens, w_gate, w_up, w_down):
    columns = w_gate.shape[1]
    rows, features = tokens.shape
    mp, dp, guide = (lax.axis_size(axis) for axis in ("mp", "dp", "guide"))
    core = lax.axis_index("guide")
    head = 2 * rows // 3
    tail = rows - head
    own_parity = lax.axis_index("mp") % guide == core
    other_tokens = from_other_core(tokens)
    both = jnp.stack([tokens, other_tokens])
    own_weights = lax.optimization_barrier(jnp.concatenate([w_gate, w_up], axis=1))
    other_weights = from_other_core(own_weights)
    other_w_down = from_other_core(w_down)
    owned = jnp.where(
        own_parity,
        both[:, :head],
        jnp.pad(both[:, head:], ((0, 0), (0, head - tail), (0, 0))),
    )
    blocks = lax.all_gather(owned.reshape(-1, features), "mp", axis=0, tiled=True)
    blocks = blocks.reshape(dp, guide, 2, head, features)
    heads = lax.dynamic_index_in_dim(blocks, core, 1, keepdims=False)
    tails = lax.dynamic_index_in_dim(blocks, 1 - core, 1, keepdims=False)[:, :, :tail]
    mine = jnp.concatenate([heads, tails], axis=2)
    chip_terms = jnp.dot(
        mine[:, 0].reshape(-1, features), own_weights, preferred_element_type=jnp.float32
    ) + jnp.dot(
        mine[:, 1].reshape(-1, features), other_weights, preferred_element_type=jnp.float32
    )
    summed = summed_on_arrival(chip_terms.astype(jnp.bfloat16).reshape(dp, rows, -1), "dp")
    hidden_share = (jax.nn.silu(summed[:, :columns]) * summed[:, columns:]).astype(jnp.bfloat16)
    copies = jnp.broadcast_to(hidden_share[None], (dp, *hidden_share.shape))
    hidden = lax.all_to_all(copies, "dp", 0, 0, tiled=True).reshape(dp * rows, columns)
    hidden, core = lax.optimization_barrier((hidden, core))
    halves = jnp.stack(
        [
            jnp.dot(hidden, w, preferred_element_type=jnp.float32)
            .astype(jnp.bfloat16)
            .reshape(dp, rows, -1)
            for w in (w_down, other_w_down)
        ],
        axis=1,
    )
    heads = halves[:, :, :head]
    tails = jnp.pad(halves[:, :, head:], ((0, 0), (0, 0), (0, head - tail), (0, 0)))
    tiles = jnp.stack(
        [jnp.where(core == parity, heads, tails) for parity in range(guide)], axis=1
    )
    output_rows = summed_on_arrival(tiles.reshape(mp, 2 * head, -1), "mp").astype(jnp.bfloat16)
    kept, received = output_rows[:head], from_other_core(output_rows[head:])
    return jnp.where(
        own_parity,
        jnp.concatenate([kept, received[:tail]], axis=0),
        jnp.concatenate([received, kept[:tail]], axis=0),
    )


def solution(mesh):
    placed = (
        P(("groups", "mp"), ("dp", "guide")),
        P(("dp", "guide"), "mp"),
        P(("dp", "guide"), "mp"),
        P("mp", ("dp", "guide")),
    )
    return jax.shard_map(
        per_device,
        mesh=mesh,
        in_specs=placed,
        out_specs=P(("groups", "mp"), ("dp", "guide")),
        check_vma=False,
    )
```
